32 devices in a mesh: asset: 8 (over z, y), tm: 4 (over x, core).
Axes of the slice: x: 2, y: 2, z: 4, core: 2. Of those that a mesh axis runs over, the one named last changes fastest.
Arguments:
- values: float32 [4, 1024, 16384], P(None, 'tm', 'asset'), may hold values from -64 to 64
- listed_from: int32 [16384], P('asset'), may hold values from -1024 to 1023, as said below
- listed_until: int32 [16384], P('asset'), may hold values from -960 to 3070, as said below
Outputs:
- standardized: float32 [4, 1024, 16384], P(None, 'tm', 'asset')
The draws below stay inside these ranges and needn't reach their ends.
Inputs may be any that keep to these rules, and one draw needn't show every extreme that they name: listed_until[a] - listed_from[a] is at least 64. listed_until[a] - listed_from[a] is at least 64.
All inputs are finite; a program needn't handle non-finite values.
Results may differ from the reference program's by a relative error of at most 0.00005.
Values sent between devices are 32-bit elements; how exact they have to be, the bound alone decides.
A program may use at most 128 MiB of HBM per device.

```python
import jax
import jax.numpy as jnp
from jax import lax

F = 4
WINDOW = 64
TIME = 1024
ASSETS = 16384


def listing_dates(key):
    base = jax.random.fold_in(key, 7)
    key_start, key_length = jax.random.split(base)
    first_stamp = jax.random.randint(key_start, (ASSETS,), -TIME, TIME, dtype=jnp.int32)
    length = jax.random.randint(key_length, (ASSETS,), WINDOW, 2 * TIME, dtype=jnp.int32)
    return (first_stamp, first_stamp + length)


def draw_listed_from(key, part):
    return listing_dates(key)[0]


def draw_listed_until(key, part):
    return listing_dates(key)[1]


def draw_values(key, part):
    base = jax.random.fold_in(key, 11)
    key_noise, key_scale, key_common, key_drift = jax.random.split(base, 4)
    noise_draw = jax.random.normal(key_noise, (F, TIME, ASSETS), jnp.float32)
    field_values = 8.0 * noise_draw
    return jnp.clip(field_values, -64.0, 64.0)


def setup_inputs(seed: int = 0) -> dict:
    arg_keys = jax.random.split(jax.random.key(seed), 4)
    values = draw_values(jax.random.fold_in(arg_keys[3], 71), 0)
    listed_from = draw_listed_from(jax.random.fold_in(arg_keys[3], 71), 0)
    listed_until = draw_listed_until(jax.random.fold_in(arg_keys[3], 71), 0)
    return {"values": values, "listed_from": listed_from, "listed_until": listed_until}


def standardize(field_values, weight, present):
    center = lax.optimization_barrier(jnp.sum(weight * field_values, axis=1)) / present
    deviate = (field_values - center[:, None]) * weight
    spread = lax.optimization_barrier(jnp.sum(deviate * deviate, axis=1)) / present
    return deviate / jnp.sqrt(spread + 0.1)[:, None]

def reference(values, listed_from, listed_until):
    stamps = jnp.arange(TIME, dtype=jnp.int32)[:, None]
    opened = listed_from[None, :]
    closed = listed_until[None, :]
    weight = ((stamps >= opened) & (stamps < closed)).astype(values.dtype)
    window_low = jnp.maximum(jnp.maximum(stamps - (WINDOW - 1), opened), 0)
    window_high = jnp.minimum(stamps, closed - 1)
    counted = jnp.maximum(window_high - window_low + 1, 1).astype(values.dtype)
    present = jnp.maximum(lax.optimization_barrier(jnp.sum(weight, axis=1)), 1.0)

    def one_field(field_values):
        window_sum = lax.reduce_window(field_values * weight, jnp.zeros((), field_values.dtype), lax.add, (WINDOW, 1), (1, 1), ((WINDOW - 1, 0), (0, 0)))
        rolling = window_sum / counted
        clipped = jnp.clip(standardize(rolling, weight, present), -3.0, 3.0)
        return standardize(clipped, weight, present)
    return lax.map(one_field, values)
```

```python
import functools

import jax
import jax.numpy as jnp
from jax import lax
from jax.experimental import pallas as pl
from jax.experimental.pallas import tpu as pltpu
from jax.sharding import PartitionSpec as P

WINDOW = 64
LANES = 128
CLIP = 3.0


def kernel(
    n_tm, n_as, values, opened_ref, closed_ref, out,
    x, weight, inverse, part1, part2, total1, total2, got1, got2, tail_part, tail_got,
    load_sem, halo_send, halo_recv, send_sem, recv_sem,
):
    fields, rows, assets = values.shape
    blocks = rows // WINDOW
    chunks = assets // LANES
    items = (blocks - 1) * fields
    tm = lax.axis_index("tm")
    me = lax.axis_index("asset")
    later = lax.rem(tm + 1, n_tm)
    before = lax.rem(tm + n_tm - 1, n_tm)

    loads = [
        pltpu.make_async_copy(values.at[f], x.at[f, pl.ds(WINDOW, rows)], load_sem.at[f])
        for f in range(fields)
    ]
    for copy in loads:
        copy.start()

    barrier = pltpu.get_barrier_semaphore()
    for other in (later, before):
        pl.semaphore_signal(barrier, inc=1, device_id={"tm": other})
    for d in range(1, n_as):
        pl.semaphore_signal(barrier, inc=1, device_id={"asset": lax.rem(me + d, n_as)})
    pl.semaphore_wait(barrier, n_as + 1)

    halos = [
        pltpu.make_async_remote_copy(
            src_ref=values.at[f, pl.ds(rows - WINDOW, WINDOW)],
            dst_ref=x.at[f, pl.ds(0, WINDOW)],
            send_sem=halo_send.at[f],
            recv_sem=halo_recv.at[f],
            device_id={"tm": later},
        )
        for f in range(fields)
    ]
    for copy in halos:
        copy.start()

    def send(part, got, stage):
        for d in range(1, n_as):
            pltpu.make_async_remote_copy(
                src_ref=part,
                dst_ref=got.at[d - 1],
                send_sem=send_sem.at[stage],
                recv_sem=recv_sem.at[stage],
                device_id={"asset": lax.rem(me + d, n_as)},
            ).start()

    def receive(part, got, stage):
        pltpu.make_async_copy(got, got, recv_sem.at[stage]).wait()
        return part[...] + jnp.sum(got[...], axis=0)

    def row_of(first, second):
        return jnp.sum(jnp.concatenate([first, second], axis=0).T, axis=0, keepdims=True)

    def factors(row, count):
        mean = row / jnp.maximum(count, 1.0)
        other = pltpu.roll(mean, WINDOW, 1)
        scale = 1.0 / jnp.sqrt(jnp.maximum(mean - other * other, 0.0) + 0.1)
        lane = lax.broadcasted_iota(jnp.int32, row.shape, 1)
        both = jnp.broadcast_to(jnp.where(lane < WINDOW, mean, scale), (LANES, LANES)).T
        return both[:WINDOW], both[WINDOW:]

    zero = jnp.zeros((WINDOW, LANES), jnp.float32)
    first_stamp = tm * rows - WINDOW

    @pl.loop(0, chunks)
    def listing(c):
        cols = pl.ds(pl.multiple_of(c * LANES, LANES), LANES)
        opened = jnp.maximum(opened_ref[:, cols], 0)
        closed = closed_ref[:, cols]

        @pl.loop(0, blocks + 1)
        def block(b):
            start = pl.multiple_of(b * WINDOW, WINDOW)
            stamps = first_stamp + start + lax.broadcasted_iota(jnp.int32, (WINDOW, LANES), 0)
            listed = (stamps >= opened) & (stamps < closed)
            low = jnp.maximum(stamps - (WINDOW - 1), opened)
            high = jnp.minimum(stamps, closed - 1)
            counted = jnp.maximum(high - low + 1, 1).astype(jnp.float32)
            weight[pl.ds(start, WINDOW), cols] = jnp.where(listed, 1.0, 0.0)
            inverse[pl.ds(start, WINDOW), cols] = jnp.where(listed, 1.0 / counted, 0.0)

    @pl.loop(0, blocks)
    def counting(b):
        def chunk(c, total):
            cols = pl.ds(pl.multiple_of(c * LANES, LANES), LANES)
            return total + weight[pl.ds(pl.multiple_of((b + 1) * WINDOW, WINDOW), WINDOW), cols]

        total = lax.fori_loop(0, chunks, chunk, zero)
        part1[pl.ds(items + b, 1), :] = row_of(total, total)

    def roll_window(f, b):
        top = pl.multiple_of(b * WINDOW, WINDOW)

        def chunk(c, carry):
            cols = pl.ds(pl.multiple_of(c * LANES, LANES), LANES)
            reach = pl.ds(top, 2 * WINDOW)
            sums = x[f, reach, cols] * weight[reach, cols]
            for step in (8, 16, 32):
                sums = sums[step:] + sums[:-step]
            for step in (1, 2, 4):
                sums = sums + pltpu.roll(sums, step, 0)
            rolling = sums[8:] * inverse[pl.ds(top + WINDOW, WINDOW), cols]
            out[f, pl.ds(top, WINDOW), cols] = rolling
            return carry[0] + rolling, carry[1] + rolling * rolling

        return row_of(*lax.fori_loop(0, chunks, chunk, (zero, zero), unroll=2))

    def clip_scores(f, b, center, scale):
        top = pl.multiple_of(b * WINDOW, WINDOW)

        def chunk(c, carry):
            cols = pl.ds(pl.multiple_of(c * LANES, LANES), LANES)
            here = pl.ds(top, WINDOW)
            scored = (out[f, here, cols] - center) * scale
            clipped = jnp.minimum(jnp.maximum(scored, -CLIP), CLIP)
            out[f, here, cols] = clipped
            masked = clipped * weight[pl.ds(top + WINDOW, WINDOW), cols]
            return carry[0] + masked, carry[1] + masked * masked

        return row_of(*lax.fori_loop(0, chunks, chunk, (zero, zero), unroll=2))

    def finish(f, b, center, scale):
        top = pl.multiple_of(b * WINDOW, WINDOW)

        @pl.loop(0, chunks, unroll=2)
        def chunk(c):
            cols = pl.ds(pl.multiple_of(c * LANES, LANES), LANES)
            here = pl.ds(top, WINDOW)
            deviate = (out[f, here, cols] - center) * weight[pl.ds(top + WINDOW, WINDOW), cols]
            out[f, here, cols] = deviate * scale

    for f in range(fields):
        loads[f].wait()

        @pl.loop(1, blocks)
        def windows(b):
            part1[pl.ds((b - 1) * fields + f, 1), :] = roll_window(f, b)

    send(part1, got1, 0)

    def main_second():
        total1[...] = receive(part1, got1, 0)

        @pl.loop(0, items)
        def item(i):
            b = lax.div(i, fields) + 1
            f = lax.rem(i, fields)
            count = total1[pl.ds(items + b, 1), :]
            center, scale = factors(total1[pl.ds(i, 1), :], count)
            part2[pl.ds(i, 1), :] = clip_scores(f, b, center, scale)

        send(part2, got2, 1)

    def main_third():
        total2[...] = receive(part2, got2, 1)

        @pl.loop(0, items)
        def item(i):
            b = lax.div(i, fields) + 1
            f = lax.rem(i, fields)
            count = total1[pl.ds(items + b, 1), :]
            center, scale = factors(total2[pl.ds(i, 1), :], count)
            finish(f, b, center, scale)

    def tail_first(f):
        halos[f].wait_recv()
        tail_part[2 * f] = jnp.broadcast_to(roll_window(f, 0), (8, LANES))
        send(tail_part.at[2 * f], tail_got.at[2 * f], 2 + 2 * f)

    def tail_factors(f, part):
        slot = 2 * f + part
        row = receive(tail_part.at[slot], tail_got.at[slot], 2 + slot)[:1]
        return factors(row, total1[pl.ds(items, 1), :])

    def tail_second(f):
        row = clip_scores(f, 0, *tail_factors(f, 0))
        tail_part[2 * f + 1] = jnp.broadcast_to(row, (8, LANES))
        send(tail_part.at[2 * f + 1], tail_got.at[2 * f + 1], 3 + 2 * f)

    def tail_third(f):
        finish(f, 0, *tail_factors(f, 1))

    tail_first(0)
    main_second()
    if fields > 1:
        tail_first(1)
    tail_second(0)
    main_third()
    for f in range(2, fields):
        tail_first(f)
        tail_second(f - 1)
        tail_third(f - 2)
    if fields > 1:
        tail_second(fields - 1)
        tail_third(fields - 2)
    tail_third(fields - 1)

    for copy in halos:
        copy.wait_send()
    pltpu.make_async_copy(got1, got1, send_sem.at[0]).wait()
    pltpu.make_async_copy(got2, got2, send_sem.at[1]).wait()
    for slot in range(2 * fields):
        got = tail_got.at[slot]
        pltpu.make_async_copy(got, got, send_sem.at[2 + slot]).wait()


def per_device(n_tm, n_as, values, listed_from, listed_until):
    fields, rows, assets = values.shape
    blocks = rows // WINDOW
    stats = -(-((blocks - 1) * fields + blocks) // 8) * 8
    f32 = jnp.float32
    vmem = pltpu.VMEM
    dma = pltpu.SemaphoreType.DMA
    return pl.pallas_call(
        functools.partial(kernel, n_tm, n_as),
        out_shape=vmem((fields, rows, assets), f32),
        in_specs=[
            pl.BlockSpec(memory_space=pl.ANY),
            pl.BlockSpec(memory_space=vmem),
            pl.BlockSpec(memory_space=vmem),
        ],
        out_specs=pl.BlockSpec(memory_space=vmem),
        scratch_shapes=[
            vmem((fields, WINDOW + rows, assets), f32),
            vmem((WINDOW + rows, assets), f32),
            vmem((WINDOW + rows, assets), f32),
            vmem((stats, LANES), f32),
            vmem((stats, LANES), f32),
            vmem((stats, LANES), f32),
            vmem((stats, LANES), f32),
            vmem((n_as - 1, stats, LANES), f32),
            vmem((n_as - 1, stats, LANES), f32),
            vmem((2 * fields, 8, LANES), f32),
            vmem((2 * fields, n_as - 1, 8, LANES), f32),
            dma((fields,)),
            dma((fields,)),
            dma((fields,)),
            dma((2 + 2 * fields,)),
            dma((2 + 2 * fields,)),
        ],
        compiler_params=pltpu.CompilerParams(
            collective_id=0, has_side_effects=True, vmem_limit_bytes=40 * 2**20
        ),
    )(values, listed_from[None], listed_until[None])


def solution(mesh):
    in_specs = (P(None, "tm", "asset"), P("asset"), P("asset"))
    out_specs = P(None, "tm", "asset")
    body = functools.partial(per_device, mesh.shape["tm"], mesh.shape["asset"])
    return jax.shard_map(
        body, mesh=mesh, in_specs=in_specs, out_specs=out_specs, check_vma=False
    )
```

```python
import functools

import jax
import jax.numpy as jnp
from jax import lax
from jax.experimental import pallas as pl
from jax.experimental.pallas import tpu as pltpu
from jax.sharding import PartitionSpec as P

WINDOW = 64
LANES = 128
CLIP = 3.0
UNROLL = 4


def field_groups(fields):
    half = (fields + 1) // 2
    return [(start, min(half, fields - start)) for start in range(0, fields, half)]


def kernel(
    n_tm, n_as, values, opened_hbm, closed_hbm, out,
    x, rolling, weight, inverse, opened_ref, closed_ref, part, got, totals,
    load_sem, halo_send, halo_recv, send_sem, recv_sem,
):
    fields, rows, assets = values.shape
    blocks = rows // WINDOW
    chunks = assets // LANES
    groups = field_groups(fields)
    tm = lax.axis_index("tm")
    me = lax.axis_index("asset")
    later = lax.rem(tm + 1, n_tm)
    before = lax.rem(tm + n_tm - 1, n_tm)

    dates = [
        pltpu.make_async_copy(opened_hbm, opened_ref, load_sem.at[fields]),
        pltpu.make_async_copy(closed_hbm, closed_ref, load_sem.at[fields + 1]),
    ]
    loads = [
        pltpu.make_async_copy(values.at[f], x.at[f, pl.ds(WINDOW, rows)], load_sem.at[f])
        for f in range(fields)
    ]

    barrier = pltpu.get_barrier_semaphore()
    for other in (later, before):
        pl.semaphore_signal(barrier, inc=1, device_id={"tm": other})
    for d in range(1, n_as):
        pl.semaphore_signal(barrier, inc=1, device_id={"asset": lax.rem(me + d, n_as)})
    for copy in dates + loads:
        copy.start()
    pl.semaphore_wait(barrier, n_as + 1)

    halos = [
        pltpu.make_async_remote_copy(
            src_ref=values.at[f, pl.ds(rows - WINDOW, WINDOW)],
            dst_ref=x.at[f, pl.ds(0, WINDOW)],
            send_sem=halo_send.at[f],
            recv_sem=halo_recv.at[f],
            device_id={"tm": later},
        )
        for f in range(fields)
    ]
    for copy in halos:
        copy.start()

    def send(slot):
        for d in range(1, n_as):
            pltpu.make_async_remote_copy(
                src_ref=part.at[slot],
                dst_ref=got.at[slot, d - 1],
                send_sem=send_sem.at[slot],
                recv_sem=recv_sem.at[slot],
                device_id={"asset": lax.rem(me + d, n_as)},
            ).start()

    def receive(slot):
        arrived = got.at[slot]
        pltpu.make_async_copy(arrived, arrived, recv_sem.at[slot]).wait()
        return part[slot] + jnp.sum(got[slot], axis=0)

    def row_of(first, second):
        return jnp.sum(jnp.concatenate([first, second], axis=0).T, axis=0, keepdims=True)

    def factors(row, count):
        mean = row / jnp.maximum(count, 1.0)
        other = pltpu.roll(mean, WINDOW, 1)
        scale = 1.0 / jnp.sqrt(jnp.maximum(mean - other * other, 0.0) + 0.1)
        lane = lax.broadcasted_iota(jnp.int32, row.shape, 1)
        both = jnp.broadcast_to(jnp.where(lane < WINDOW, mean, scale), (LANES, LANES)).T
        return both[:WINDOW], both[WINDOW:]

    def columns(c):
        return pl.ds(pl.multiple_of(c * LANES, LANES), LANES)

    zero = jnp.zeros((WINDOW, LANES), jnp.float32)
    part[...] = jnp.zeros(part.shape, part.dtype)
    first_stamp = tm * rows - WINDOW
    for copy in dates:
        copy.wait()

    @pl.loop(0, blocks + 1)
    def listing(b):
        start = pl.multiple_of(b * WINDOW, WINDOW)
        stamps = first_stamp + start + lax.broadcasted_iota(jnp.int32, (WINDOW, LANES), 0)

        def chunk(c, total):
            cols = columns(c)
            opened = jnp.maximum(opened_ref[:, cols], 0)
            closed = closed_ref[:, cols]
            listed = (stamps >= opened) & (stamps < closed)
            low = jnp.maximum(stamps - (WINDOW - 1), opened)
            counted = jnp.maximum(jnp.minimum(stamps + 1, closed) - low, 1).astype(jnp.float32)
            ones = jnp.where(listed, 1.0, 0.0)
            weight[pl.ds(start, WINDOW), cols] = ones
            inverse[pl.ds(start, WINDOW), cols] = ones / counted
            return total + ones

        total = lax.fori_loop(0, chunks, chunk, zero, unroll=2)
        part[0, pl.ds(lax.rem(b + blocks, blocks + 1), 1), :] = row_of(total, total)

    send(0)

    def roll_window(f, b):
        top = pl.multiple_of(b * WINDOW, WINDOW)

        def chunk(c, carry):
            cols = columns(c)
            reach = pl.ds(top, 2 * WINDOW)
            sums = x[f, reach, cols] * weight[reach, cols]
            for step in (8, 16, 32):
                sums = sums[step:] + sums[:-step]
            for step in (1, 2, 4):
                sums = sums + pltpu.roll(sums, step, 0)
            means = sums[8:] * inverse[pl.ds(top + WINDOW, WINDOW), cols]
            rolling[f, pl.ds(top, WINDOW), cols] = means
            return carry[0] + means, carry[1] + means * means

        return row_of(*lax.fori_loop(0, chunks, chunk, (zero, zero), unroll=UNROLL))

    def clip_scores(f, b, center, scale):
        top = pl.multiple_of(b * WINDOW, WINDOW)

        def chunk(c, carry):
            cols = columns(c)
            scored = (rolling[f, pl.ds(top, WINDOW), cols] - center) * scale
            clipped = jnp.minimum(jnp.maximum(scored, -CLIP), CLIP)
            masked = clipped * weight[pl.ds(top + WINDOW, WINDOW), cols]
            return carry[0] + masked, carry[1] + masked * clipped

        return row_of(*lax.fori_loop(0, chunks, chunk, (zero, zero), unroll=UNROLL))

    def finish(f, b, first, second):
        top = pl.multiple_of(b * WINDOW, WINDOW)
        center, scale = first
        middle, factor = second

        @pl.loop(0, chunks, unroll=UNROLL)
        def chunk(c):
            cols = columns(c)
            here = pl.ds(top, WINDOW)
            scored = (rolling[f, here, cols] - center) * scale
            clipped = jnp.minimum(jnp.maximum(scored, -CLIP), CLIP)
            deviate = (clipped - middle) * weight[pl.ds(top + WINDOW, WINDOW), cols]
            out[f, here, cols] = deviate * factor

    def count_row(b):
        return totals[0, pl.ds(b, 1), :]

    def total_row(slot, i):
        return totals[slot, pl.ds(i, 1), :]

    def main_first(g):
        start, size = groups[g]
        for f in range(start, start + size):
            loads[f].wait()

        @pl.loop(0, size * (blocks - 1))
        def item(i):
            f, b = start + lax.rem(i, size), 1 + lax.div(i, size)
            part[1 + 2 * g, pl.ds(i, 1), :] = roll_window(f, b)

        send(1 + 2 * g)

    def main_second(g):
        start, size = groups[g]
        slot = 1 + 2 * g
        totals[slot] = receive(slot)

        @pl.loop(0, size * (blocks - 1))
        def item(i):
            f, b = start + lax.rem(i, size), 1 + lax.div(i, size)
            center, scale = factors(total_row(slot, i), count_row(b))
            part[slot + 1, pl.ds(i, 1), :] = clip_scores(f, b, center, scale)

        send(slot + 1)

    def main_third(g):
        start, size = groups[g]
        slot = 1 + 2 * g
        totals[slot + 1] = receive(slot + 1)

        @pl.loop(0, size * (blocks - 1))
        def item(i):
            f, b = start + lax.rem(i, size), 1 + lax.div(i, size)
            count = count_row(b)
            first = factors(total_row(slot, i), count)
            finish(f, b, first, factors(total_row(slot + 1, i), count))

    tail_slot = 1 + 2 * len(groups)

    def tail_first(f):
        slot = tail_slot + 2 * f
        halos[f].wait_recv()
        part[slot, :1, :] = roll_window(f, 0)
        send(slot)

    def tail_second(f):
        slot = tail_slot + 2 * f
        totals[slot] = receive(slot)
        center, scale = factors(total_row(slot, 0), count_row(0))
        part[slot + 1, :1, :] = clip_scores(f, 0, center, scale)
        send(slot + 1)

    def tail_third(f):
        slot = tail_slot + 2 * f
        totals[slot + 1] = receive(slot + 1)
        first = factors(total_row(slot, 0), count_row(0))
        finish(f, 0, first, factors(total_row(slot + 1, 0), count_row(0)))

    early = min(2, fields)
    for g in range(len(groups)):
        main_first(g)
    totals[0] = receive(0)
    for step in range(max(early, len(groups))):
        if step < early:
            tail_first(step)
        if step < len(groups):
            main_second(step)
    for step in range(max(early, len(groups))):
        if step < early:
            tail_second(step)
        if step < len(groups):
            main_third(step)
    for f in range(early, fields):
        tail_first(f)
        if f > early:
            tail_second(f - 1)
        tail_third(f - early)
    if fields > early:
        tail_second(fields - 1)
    for f in range(fields - early, fields):
        tail_third(f)

    for copy in halos:
        copy.wait_send()
    for slot in range(part.shape[0]):
        sent = got.at[slot]
        pltpu.make_async_copy(sent, sent, send_sem.at[slot]).wait()


def per_device(n_tm, n_as, values, listed_from, listed_until):
    fields, rows, assets = values.shape
    blocks = rows // WINDOW
    groups = field_groups(fields)
    stats = -(-max(groups[0][1] * (blocks - 1), blocks + 1) // 8) * 8
    slots = 1 + 2 * len(groups) + 2 * fields
    f32 = jnp.float32
    vmem = pltpu.VMEM
    dma = pltpu.SemaphoreType.DMA
    return pl.pallas_call(
        functools.partial(kernel, n_tm, n_as),
        out_shape=vmem((fields, rows, assets), f32),
        in_specs=[pl.BlockSpec(memory_space=pltpu.HBM)] * 3,
        out_specs=pl.BlockSpec(memory_space=vmem),
        scratch_shapes=[
            vmem((fields, WINDOW + rows, assets), f32),
            vmem((fields, rows, assets), f32),
            vmem((WINDOW + rows, assets), f32),
            vmem((WINDOW + rows, assets), f32),
            vmem((1, assets), jnp.int32),
            vmem((1, assets), jnp.int32),
            vmem((slots, stats, LANES), f32),
            vmem((slots, n_as - 1, stats, LANES), f32),
            vmem((slots, stats, LANES), f32),
            dma((fields + 2,)),
            dma((fields,)),
            dma((fields,)),
            dma((slots,)),
            dma((slots,)),
        ],
        compiler_params=pltpu.CompilerParams(
            collective_id=0, has_side_effects=True, vmem_limit_bytes=48 * 2**20
        ),
    )(values, listed_from[None], listed_until[None])


def solution(mesh):
    in_specs = (P(None, "tm", "asset"), P("asset"), P("asset"))
    out_specs = P(None, "tm", "asset")
    body = functools.partial(per_device, mesh.shape["tm"], mesh.shape["asset"])
    return jax.shard_map(
        body, mesh=mesh, in_specs=in_specs, out_specs=out_specs, check_vma=False
    )
```
